1024 devices in a mesh: sub: 16 (over z, core), wide: 64 (over y, x).
Axes of the slice: x: 8, y: 8, z: 8, core: 2. Of those that a mesh axis runs over, the one named last changes fastest.
Arguments:
- load_table: bfloat16 [16, 64, 16, 4, 128], P('sub', 'wide'), may hold values from -6 to 6
- load_column: int32 [64], replicated, may hold values from 0 to 15
- face_order: int32 [16, 64, 4], P('sub', 'wide'), may hold values from 0 to 3, each once within a row
- schur: bfloat16 [16, 64, 512, 512], P('sub', 'wide'), as said below
- neumann: bfloat16 [16, 64, 512, 512], P('sub', 'wide'), as said below
- coarse_basis: bfloat16 [16, 64, 4, 4, 128], P('sub', 'wide'), may hold values from -0.625 to 0.625
- corner_map: int32 [16, 64, 4], P('sub', 'wide'), may hold values from 0 to 1151, as said below
- coarse_inverse: float32 [1152, 1152], P('wide'), as said below
Outputs:
- solution: float32 [16, 64, 4, 64, 128], P('sub', 'wide')
The draws below stay inside these ranges and needn't reach their ends.
Inputs may be any that keep to these rules, and one draw needn't show every extreme that they name: `corner_map`: each subdomain's 4 entries are distinct; subdomains that meet at a corner of the grid of subdomains give it the same number, and different corners get different numbers, so (17) * (65) of the 1152 numbers occur and the others belong to no corner. `coarse_inverse`: Symmetric. `schur`: Symmetric. `neumann`: Symmetric.
All inputs are finite; a program needn't handle non-finite values.
Results may differ from the reference program's by a relative error of at most 0.0014.
Values sent between devices are 32-bit elements; how exact they have to be, the bound alone decides.
No kernel may reach another device: no remote copies, remote signals or barrier semaphores. Data moves between devices by JAX's collectives and lax.ppermute only.
A program may use at most 32 MiB of HBM per device.

```python
import math
import jax
import jax.numpy as jnp
from jax import lax

NI = 512
RHS = 64
NLOAD = 16
PRIM = 4
ITERS = 3
FB = 128
ROWS = 16
COLS = 64
NCOARSE = 1152


def spd_blocks(key, lowest, highest, spread):
    key_diag, key_noise = jax.random.split(key)
    diagonal = jax.random.uniform(key_diag, (ROWS, COLS, NI), jnp.float32, lowest, highest)
    noise_part = jax.random.normal(key_noise, (ROWS, COLS, NI, NI), jnp.float32) * (spread / math.sqrt(2.0 * NI))
    symmetric = noise_part + jnp.swapaxes(noise_part, 2, 3)
    identity = jnp.eye(NI, dtype=jnp.float32)
    return (symmetric + diagonal[..., None] * identity).astype(jnp.bfloat16)


def draw_schur(key, part):
    return spd_blocks(jax.random.fold_in(key, 11), 1.0, 2.0, 0.35)


def draw_neumann(key, part):
    return spd_blocks(jax.random.fold_in(key, 23), 0.6, 1.2, 0.25)


def draw_coarse_inverse(key, part):
    key_diag, key_noise = jax.random.split(jax.random.fold_in(key, 37))
    lowest, highest, spread = (0.6, 1.2, 0.2)
    diagonal = jax.random.uniform(key_diag, (NCOARSE,), jnp.float32, lowest, highest)
    noise_part = jax.random.normal(key_noise, (NCOARSE, NCOARSE), jnp.float32) * (spread / math.sqrt(1.0 * NCOARSE))
    symmetric = noise_part + noise_part.T
    return symmetric + jnp.diag(diagonal)


def draw_corner_map(key, part):
    numbering = jax.random.permutation(jax.random.fold_in(key, 53), NCOARSE)
    corner_base = jnp.arange(ROWS)[:, None] * (COLS + 1) + jnp.arange(COLS)[None, :]
    corner_index = jnp.stack([corner_base, corner_base + 1, corner_base + COLS + 1, corner_base + COLS + 2], axis=-1)
    return numbering[corner_index].astype(jnp.int32)


def place_ends(array, stream_key, low, top_value):
    longest = array.shape.index(max(array.shape))
    spots = []
    for shift in (0, 1):
        where = [jax.random.randint(jax.random.fold_in(stream_key, axis), (), 0, length) for axis, length in enumerate(array.shape)]
        where[longest] = (where[longest] + shift) % array.shape[longest]
        spots.append(tuple(where))
    return array.at[spots[0]].set(low).at[spots[1]].set(top_value)


def level_of(stream_key, shape, cuts, smallest, largest):
    def one(position, shards_of):
        draws = jax.random.uniform(jax.random.fold_in(jax.random.fold_in(stream_key, 6), position), (shards_of,), jnp.float32, smallest / len(cuts), largest / len(cuts))
        return jnp.repeat(jnp.exp(draws), shape[position] // shards_of).reshape((-1,) + (1,) * (len(shape) - position - 1))

    gain = one(*cuts[0])
    for cut in cuts[1:]:
        gain = gain * one(*cut)
    return gain


def noise(stream_key, shape, scale, bound, cuts=(), kind=jnp.bfloat16):
    drawn = scale * jax.random.normal(stream_key, shape, jnp.float32)
    if cuts:
        drawn = drawn * level_of(stream_key, shape, cuts, -0.22, 0.18)
    return jnp.clip(drawn, -bound, bound).astype(kind)


def setup_inputs(seed: int = 0) -> dict:
    key_list = jax.random.split(jax.random.key(seed), 9)
    load_table = noise(key_list[0], (ROWS, COLS, NLOAD, 4, FB), 1.0, 6.0, ((0, 16), (1, 64)))
    load_column = place_ends(jax.random.randint(key_list[1], (RHS,), 0, NLOAD), jax.random.fold_in(key_list[1], 1), 0, NLOAD - 1).astype(jnp.int32)
    face_order = jax.vmap(lambda own: jax.random.permutation(own, 4))(jax.random.split(key_list[2], ROWS * COLS)).reshape((ROWS, COLS, 4)).astype(jnp.int32)
    schur = draw_schur(jax.random.fold_in(key_list[8], 71), 0)
    neumann = draw_neumann(jax.random.fold_in(key_list[8], 71), 0)
    coarse_basis = noise(key_list[5], (ROWS, COLS, PRIM, 4, FB), (NI // 5) ** -0.5, 0.625, ((0, 16), (1, 64)))
    corner_map = draw_corner_map(jax.random.fold_in(key_list[8], 71), 0)
    coarse_inverse = draw_coarse_inverse(jax.random.fold_in(key_list[8], 71), 0)
    return dict(load_table=load_table, load_column=load_column, face_order=face_order, schur=schur, neumann=neumann, coarse_basis=coarse_basis, corner_map=corner_map, coarse_inverse=coarse_inverse)


damping = 0.3


def share_weights():
    row_index = jnp.arange(ROWS)[:, None] * jnp.ones((1, COLS), jnp.int32)
    col_index = jnp.ones((ROWS, 1), jnp.int32) * jnp.arange(COLS)[None, :]
    half = jnp.float32(0.5)
    whole = jnp.float32(1.0)
    north_share = jnp.where(row_index > 0, half, whole)
    south_share = jnp.where(row_index < ROWS - 1, half, whole)
    west_share = jnp.where(col_index > 0, half, whole)
    east_share = jnp.where(col_index < COLS - 1, half, whole)
    return jnp.stack([north_share, south_share, west_share, east_share], axis=2)[:, :, :, None, None]


def assemble(copies):
    empty_row = jnp.zeros_like(copies[:1, :, 0])
    empty_col = jnp.zeros_like(copies[:, :1, 0])
    upper_faces = jnp.concatenate([empty_row, copies[:-1, :, 1]], axis=0)
    lower_faces = jnp.concatenate([copies[1:, :, 0], empty_row], axis=0)
    left_faces = jnp.concatenate([empty_col, copies[:, :-1, 3]], axis=1)
    right_faces = jnp.concatenate([copies[:, 1:, 2], empty_col], axis=1)
    return jnp.stack([copies[:, :, 0] + upper_faces, copies[:, :, 1] + lower_faces,
                      copies[:, :, 2] + left_faces, copies[:, :, 3] + right_faces], axis=2)


def apply_local(vectors, operators, face_order):
    selector = (face_order[..., :, None] == jnp.arange(4, dtype=jnp.int32)).astype(jnp.float32)
    rounded = lax.optimization_barrier(vectors.astype(jnp.bfloat16)).astype(jnp.float32)
    blocked = jnp.einsum('rcbf,rcfjn->rcjbn', selector, rounded, precision=lax.Precision.HIGHEST)
    blocked = blocked.reshape(ROWS * COLS, RHS, NI).astype(jnp.bfloat16)
    flat_ops = operators.reshape(ROWS * COLS, NI, NI)
    product = lax.map(lambda operands: jnp.dot(operands[0], operands[1], preferred_element_type=jnp.float32),
                      (blocked, flat_ops))
    product = product.reshape(ROWS, COLS, RHS, 4, FB)
    return jnp.einsum('rcbf,rcjbn->rcfjn', selector, product, precision=lax.Precision.HIGHEST)


def reference(load_table, load_column, face_order, schur, neumann, coarse_basis, corner_map, coarse_inverse):
    load_select = (load_column[:, None] == jnp.arange(NLOAD, dtype=jnp.int32)).astype(jnp.float32)
    load_faces = jnp.einsum('jl,rclfn->rcfjn', load_select, load_table.astype(jnp.float32),
                            precision=lax.Precision.HIGHEST)
    weights = share_weights()
    basis = coarse_basis.astype(jnp.float32)
    solution = jnp.zeros((ROWS, COLS, 4, RHS, FB), jnp.float32)
    for iteration in range(ITERS):
        if iteration == 0:
            residual = assemble(load_faces)
        else:
            residual = assemble(load_faces - apply_local(solution, schur, face_order))
        weighted = weights * residual
        restricted = jnp.einsum('rcpfn,rcfjn->rcpj', basis, weighted, precision=lax.Precision.HIGHEST)
        coarse_residual = jax.ops.segment_sum(restricted.reshape(ROWS * COLS * PRIM, RHS),
                                              corner_map.reshape(ROWS * COLS * PRIM), NCOARSE)
        coarse_solution = jnp.dot(coarse_residual.T, coarse_inverse, precision=lax.Precision.HIGHEST)
        picked = coarse_solution[:, corner_map]
        correction = jnp.einsum('jrcp,rcpfn->rcfjn', picked, basis, precision=lax.Precision.HIGHEST)
        neumann_part = apply_local(weighted, neumann, face_order)
        update = assemble(weights * (neumann_part + correction))
        solution = solution + damping * update
    return solution
```

```python
import jax
import jax.numpy as jnp
from jax import lax
from jax.sharding import PartitionSpec as P

ITERS = 3
damping = 0.3
HIGHEST = lax.Precision.HIGHEST


def assemble(faces):
    rows = lax.axis_size("sub")
    cols = lax.axis_size("wide")
    down = [(i, i + 1) for i in range(rows - 1)]
    right = [(i, i + 1) for i in range(cols - 1)]
    from_north = lax.ppermute(faces[1], "sub", down)
    from_south = lax.ppermute(faces[0], "sub", [(b, a) for a, b in down])
    from_west = lax.ppermute(faces[3], "wide", right)
    from_east = lax.ppermute(faces[2], "wide", [(b, a) for a, b in right])
    return faces + jnp.stack([from_north, from_south, from_west, from_east])


def apply_local(faces, operator, selector_half, selector_full):
    rhs, width = faces.shape[1:]
    blocked = jnp.einsum(
        "bf,fjn->jbn", selector_half, faces.astype(jnp.bfloat16), preferred_element_type=jnp.float32
    )
    blocked = blocked.astype(jnp.bfloat16).reshape(rhs, 4 * width)
    product = jnp.dot(blocked, operator, preferred_element_type=jnp.float32)
    product = product.reshape(rhs, 4, width)
    return jnp.einsum("bf,jbn->fjn", selector_full, product, precision=HIGHEST)


def in_three(array):
    high = lax.reduce_precision(array, 8, 7)
    rest = array - high
    middle = lax.reduce_precision(rest, 8, 7)
    low = lax.reduce_precision(rest - middle, 8, 7)
    return high.astype(jnp.bfloat16), middle.astype(jnp.bfloat16), low.astype(jnp.bfloat16)


def pick_columns(matrix, ids):
    parts = jnp.concatenate(in_three(matrix), axis=0)
    order = matrix.shape[1]
    marks = (jnp.arange(order, dtype=jnp.int32)[:, None] == ids[None, :]).astype(jnp.bfloat16)
    picked = jnp.dot(parts, marks, preferred_element_type=jnp.float32)
    high, middle, low = jnp.split(picked, 3, axis=0)
    return (high + middle) + low


def own_inverse_rows(corner_ids, coarse_inverse):
    peers = lax.axis_size("wide")
    owned = coarse_inverse.shape[0]
    prims = corner_ids.shape[0]
    id_row = jnp.pad(corner_ids.astype(jnp.float32), (0, 128 - prims))[None, :]
    ids = lax.all_gather(id_row, "wide")[:, 0, :prims].astype(jnp.int32).reshape(-1)
    entries = pick_columns(coarse_inverse, ids)
    entries = entries.reshape(owned, peers, prims).transpose(1, 2, 0).reshape(peers, prims * owned)
    entries = lax.all_to_all(entries, "wide", 0, 0, tiled=True)
    entries = entries.reshape(peers, prims, owned).transpose(1, 0, 2)
    return entries.reshape(prims, peers * owned)


def slots_of_column(ids, amount):
    count = ids.shape[0]
    place = jnp.arange(count, dtype=jnp.int32)
    same = ids[:, None] == ids[None, :]
    first = ~jnp.any(same & (place[None, :] < place[:, None]), axis=1)
    rank_of_first = jnp.sum(first[None, :] & (place[None, :] < place[:, None]), axis=1)
    rank = jnp.sum(jnp.where(same & first[None, :], rank_of_first[None, :], 0), axis=1)
    slots = rank[None, :] == jnp.arange(amount, dtype=jnp.int32)[:, None]
    slot_ids = jnp.max(jnp.where(slots, ids[None, :], 0.0), axis=1)
    return slots.astype(jnp.float32), slot_ids


def body(
    load_table, load_column, face_order, schur, neumann, coarse_basis, corner_map, coarse_inverse
):
    load_table, face_order, schur, neumann, coarse_basis, corner_ids = (
        a[0, 0] for a in (load_table, face_order, schur, neumann, coarse_basis, corner_map)
    )
    patterns = load_table.shape[0]
    prims = corner_ids.shape[0]
    rhs = load_column.shape[0]
    rows_total = lax.axis_size("sub")
    cols_total = lax.axis_size("wide")
    half_slots = rows_total + 1
    selector_full = (face_order[:, None] == jnp.arange(4, dtype=jnp.int32)).astype(jnp.float32)
    selector_half = selector_full.astype(jnp.bfloat16)
    load_select = (load_column[:, None] == jnp.arange(patterns, dtype=jnp.int32)).astype(
        jnp.bfloat16
    )
    load_faces = jnp.einsum(
        "jl,lfn->fjn", load_select, load_table, preferred_element_type=jnp.float32
    )
    row = lax.axis_index("sub")
    col = lax.axis_index("wide")
    inner = jnp.stack([row > 0, row < rows_total - 1, col > 0, col < cols_total - 1])
    weights = jnp.where(inner, jnp.float32(0.5), jnp.float32(1.0))[:, None, None]
    basis = coarse_basis.astype(jnp.float32)
    inverse_rows = own_inverse_rows(corner_ids, coarse_inverse)
    id_lanes = jnp.broadcast_to(corner_ids.astype(jnp.float32)[:, None], (prims, rhs))
    solution = jnp.zeros(load_faces.shape, jnp.float32)
    for iteration in range(ITERS):
        if iteration == 0:
            residual = assemble(load_faces)
        else:
            residual = assemble(
                load_faces - apply_local(solution, schur, selector_half, selector_full)
            )
        weighted = weights * residual
        restricted = jnp.einsum("pfn,fjn->pj", basis, weighted, precision=HIGHEST)
        in_column = lax.all_gather(
            jnp.concatenate([restricted, id_lanes], axis=1), "sub", axis=0, tiled=True
        )
        if iteration == 0:
            slots, slot_ids = slots_of_column(in_column[:, rhs], 2 * half_slots)
        summed = jnp.dot(slots, in_column[:, :rhs], precision=HIGHEST)
        summed = jnp.concatenate([summed[:half_slots], summed[half_slots:]], axis=1)
        if iteration == 0:
            id_row = jnp.pad(slot_ids, (0, 2 * rhs - 2 * half_slots))[None, :]
            everyone = lax.all_gather(jnp.concatenate([summed, id_row]), "wide")
            ids = everyone[:, half_slots, : 2 * half_slots].astype(jnp.int32)
            everyone = everyone[:, :half_slots]
            ids = ids.reshape(cols_total, 2, half_slots).transpose(1, 0, 2).reshape(-1)
            rows_at = pick_columns(inverse_rows, ids)
            rows_at = rows_at.reshape(prims, 2, cols_total * half_slots)
            rows_at = rows_at.transpose(1, 0, 2).reshape(2 * prims, -1)
        else:
            everyone = lax.all_gather(summed, "wide")
        solved = jnp.dot(
            rows_at, everyone.reshape(cols_total * half_slots, 2 * rhs), precision=HIGHEST
        )
        picked = solved[:prims, :rhs] + solved[prims:, rhs:]
        neumann_part = apply_local(weighted, neumann, selector_half, selector_full)
        correction = jnp.einsum("pj,pfn->fjn", picked, basis, precision=HIGHEST)
        update = assemble(weights * (neumann_part + correction))
        solution = solution + damping * update
    return solution[None, None]


def solution(mesh):
    in_specs = (
        P("sub", "wide", None, None, None),
        P(),
        P("sub", "wide", None),
        P("sub", "wide", None, None),
        P("sub", "wide", None, None),
        P("sub", "wide", None, None, None),
        P("sub", "wide", None),
        P("wide", None),
    )
    out_specs = P("sub", "wide", None, None, None)
    return jax.shard_map(body, mesh=mesh, in_specs=in_specs, out_specs=out_specs, check_vma=False)
```

```python
import jax
import jax.numpy as jnp
from jax import lax
from jax.sharding import PartitionSpec as P

ITERS = 3
damping = 0.3
HIGHEST = lax.Precision.HIGHEST


def assemble(faces):
    rows = lax.axis_size("sub")
    cols = lax.axis_size("wide")
    down = [(i, i + 1) for i in range(rows - 1)]
    right = [(i, i + 1) for i in range(cols - 1)]
    from_north = lax.ppermute(faces[1], "sub", down)
    from_south = lax.ppermute(faces[0], "sub", [(b, a) for a, b in down])
    from_west = lax.ppermute(faces[3], "wide", right)
    from_east = lax.ppermute(faces[2], "wide", [(b, a) for a, b in right])
    return faces + jnp.stack([from_north, from_south, from_west, from_east])


def apply_local(faces, operator, selector_half, selector_full):
    rhs, width = faces.shape[1:]
    blocked = jnp.einsum(
        "bf,fjn->jbn", selector_half, faces.astype(jnp.bfloat16), preferred_element_type=jnp.float32
    )
    blocked = blocked.astype(jnp.bfloat16).reshape(rhs, 4 * width)
    product = jnp.dot(blocked, operator, preferred_element_type=jnp.float32)
    product = product.reshape(rhs, 4, width)
    return jnp.einsum("bf,jbn->fjn", selector_full, product, precision=HIGHEST)


def gather(array, axis):
    peers = lax.axis_size(axis)
    copies = jnp.broadcast_to(array[None], (peers, *array.shape))
    return lax.all_to_all(copies, axis, 0, 0, tiled=True)


def in_three(array):
    high = lax.reduce_precision(array, 8, 7)
    rest = array - high
    middle = lax.reduce_precision(rest, 8, 7)
    low = lax.reduce_precision(rest - middle, 8, 7)
    return high.astype(jnp.bfloat16), middle.astype(jnp.bfloat16), low.astype(jnp.bfloat16)


def pick_columns(matrix, ids):
    parts = jnp.concatenate(in_three(matrix), axis=0)
    order = matrix.shape[1]
    marks = (jnp.arange(order, dtype=jnp.int32)[:, None] == ids[None, :]).astype(jnp.bfloat16)
    picked = jnp.dot(parts, marks, preferred_element_type=jnp.float32)
    high, middle, low = jnp.split(picked, 3, axis=0)
    return (high + middle) + low


def own_inverse_rows(corner_ids, ids, coarse_inverse):
    peers, slots = ids.shape
    owned = coarse_inverse.shape[0]
    col = lax.axis_index("wide")
    entries = pick_columns(coarse_inverse, ids.reshape(-1))
    entries = entries.reshape(owned, peers, slots).transpose(1, 0, 2)
    entries = lax.all_to_all(entries.reshape(peers, owned * slots), "wide", 0, 0, tiled=True)
    entries = entries.reshape(peers * owned, slots)
    column_ids = lax.dynamic_index_in_dim(ids, col, 0, keepdims=False)
    mine = (corner_ids[:, None] == column_ids[None, :]).astype(jnp.float32)
    return jnp.einsum("ps,ks->pk", mine, entries, precision=HIGHEST)


def slots_of_column(ids, amount):
    count = ids.shape[0]
    place = jnp.arange(count, dtype=jnp.int32)
    same = ids[:, None] == ids[None, :]
    first = ~jnp.any(same & (place[None, :] < place[:, None]), axis=1)
    rank_of_first = jnp.sum(first[None, :] & (place[None, :] < place[:, None]), axis=1)
    rank = jnp.sum(jnp.where(same & first[None, :], rank_of_first[None, :], 0), axis=1)
    slots = rank[None, :] == jnp.arange(amount, dtype=jnp.int32)[:, None]
    slot_ids = jnp.max(jnp.where(slots, ids[None, :], 0.0), axis=1)
    return slots.astype(jnp.float32), slot_ids


def body(
    load_table, load_column, face_order, schur, neumann, coarse_basis, corner_map, coarse_inverse
):
    load_table, face_order, schur, neumann, coarse_basis, corner_ids = (
        a[0, 0] for a in (load_table, face_order, schur, neumann, coarse_basis, corner_map)
    )
    patterns = load_table.shape[0]
    prims = corner_ids.shape[0]
    rhs = load_column.shape[0]
    rows_total = lax.axis_size("sub")
    cols_total = lax.axis_size("wide")
    half_slots = rows_total + 1
    selector_full = (face_order[:, None] == jnp.arange(4, dtype=jnp.int32)).astype(jnp.float32)
    selector_half = selector_full.astype(jnp.bfloat16)
    load_select = (load_column[:, None] == jnp.arange(patterns, dtype=jnp.int32)).astype(
        jnp.bfloat16
    )
    load_faces = jnp.einsum(
        "jl,lfn->fjn", load_select, load_table, preferred_element_type=jnp.float32
    )
    row = lax.axis_index("sub")
    col = lax.axis_index("wide")
    inner = jnp.stack([row > 0, row < rows_total - 1, col > 0, col < cols_total - 1])
    weights = jnp.where(inner, jnp.float32(0.5), jnp.float32(1.0))[:, None, None]
    basis = coarse_basis.astype(jnp.float32)
    id_lanes = jnp.broadcast_to(corner_ids.astype(jnp.float32)[:, None], (prims, rhs))
    solution = jnp.zeros(load_faces.shape, jnp.float32)
    for iteration in range(ITERS):
        if iteration == 0:
            residual = assemble(load_faces)
        else:
            residual = assemble(
                load_faces - apply_local(solution, schur, selector_half, selector_full)
            )
        weighted = weights * residual
        restricted = jnp.einsum("pfn,fjn->pj", basis, weighted, precision=HIGHEST)
        in_column = gather(jnp.concatenate([restricted, id_lanes], axis=1), "sub")
        in_column = in_column.reshape(rows_total * prims, 2 * rhs)
        if iteration == 0:
            slots, slot_ids = slots_of_column(in_column[:, rhs], 2 * half_slots)
        summed = jnp.dot(slots, in_column[:, :rhs], precision=HIGHEST)
        summed = jnp.concatenate([summed[:half_slots], summed[half_slots:]], axis=1)
        if iteration == 0:
            id_row = jnp.pad(slot_ids, (0, 2 * rhs - 2 * half_slots))[None, :]
            everyone = gather(jnp.concatenate([summed, id_row]), "wide")
            ids = everyone[:, half_slots, : 2 * half_slots].astype(jnp.int32)
            everyone = everyone[:, :half_slots]
            inverse_rows = own_inverse_rows(corner_ids, ids, coarse_inverse)
            ids = ids.reshape(cols_total, 2, half_slots).transpose(1, 0, 2).reshape(-1)
            rows_at = pick_columns(inverse_rows, ids)
            rows_at = rows_at.reshape(prims, 2, cols_total * half_slots)
            rows_at = rows_at.transpose(1, 0, 2).reshape(2 * prims, -1)
        else:
            everyone = gather(summed, "wide")
        solved = jnp.dot(
            rows_at, everyone.reshape(cols_total * half_slots, 2 * rhs), precision=HIGHEST
        )
        picked = solved[:prims, :rhs] + solved[prims:, rhs:]
        neumann_part = apply_local(weighted, neumann, selector_half, selector_full)
        correction = jnp.einsum("pj,pfn->fjn", picked, basis, precision=HIGHEST)
        update = assemble(weights * (neumann_part + correction))
        solution = solution + damping * update
    return solution[None, None]


def solution(mesh):
    in_specs = (
        P("sub", "wide", None, None, None),
        P(),
        P("sub", "wide", None),
        P("sub", "wide", None, None),
        P("sub", "wide", None, None),
        P("sub", "wide", None, None, None),
        P("sub", "wide", None),
        P("wide", None),
    )
    out_specs = P("sub", "wide", None, None, None)
    return jax.shard_map(body, mesh=mesh, in_specs=in_specs, out_specs=out_specs, check_vma=False)
```

```python
import jax
import jax.numpy as jnp
from jax import lax
from jax.sharding import PartitionSpec as P

ITERS = 3
damping = 0.3
HIGHEST = lax.Precision.HIGHEST


def pairs(axis, first):
    peers = lax.axis_size(axis)
    lower = range(first, peers - 1, 2)
    return [(i, i + 1) for i in lower] + [(i + 1, i) for i in lower]


def swap_across(low, high, axis):
    even = lax.axis_index(axis) % 2 == 0
    shifted = lax.ppermute(jnp.where(even, low, high), axis, pairs(axis, 1))
    paired = lax.ppermute(jnp.where(even, high, low), axis, pairs(axis, 0))
    return jnp.where(even, shifted, paired), jnp.where(even, paired, shifted)


def partners(faces):
    west, east = swap_across(faces[2], faces[3], "wide")
    north, south = swap_across(faces[0], faces[1], "sub")
    return jnp.stack([north, south, west, east])


def assemble(faces):
    return faces + partners(faces)


def apply_local(faces, operator, selector_half, selector_full):
    rhs, width = faces.shape[1:]
    blocked = jnp.einsum(
        "bf,fjn->jbn", selector_half, faces.astype(jnp.bfloat16), preferred_element_type=jnp.float32
    )
    blocked = blocked.astype(jnp.bfloat16).reshape(rhs, 4 * width)
    product = jnp.dot(blocked, operator, preferred_element_type=jnp.float32)
    product = product.reshape(rhs, 4, width)
    return jnp.einsum("bf,jbn->fjn", selector_full, product, precision=HIGHEST)


def gather(array, axis):
    peers = lax.axis_size(axis)
    copies = jnp.broadcast_to(array[None], (peers, *array.shape))
    return lax.all_to_all(copies, axis, 0, 0, tiled=True)


def in_three(array):
    high = lax.reduce_precision(array, 8, 7)
    rest = array - high
    middle = lax.reduce_precision(rest, 8, 7)
    low = lax.reduce_precision(rest - middle, 8, 7)
    return high.astype(jnp.bfloat16), middle.astype(jnp.bfloat16), low.astype(jnp.bfloat16)


def pick_columns(matrix, ids):
    parts = jnp.concatenate(in_three(matrix), axis=0)
    order = matrix.shape[1]
    marks = (jnp.arange(order, dtype=jnp.int32)[:, None] == ids[None, :]).astype(jnp.bfloat16)
    picked = jnp.dot(parts, marks, preferred_element_type=jnp.float32)
    high, middle, low = jnp.split(picked, 3, axis=0)
    return (high + middle) + low


def own_inverse_rows(corner_ids, ids, coarse_inverse):
    peers, slots = ids.shape
    owned = coarse_inverse.shape[0]
    col = lax.axis_index("wide")
    entries = pick_columns(coarse_inverse, ids.reshape(-1))
    entries = entries.reshape(owned, peers, slots).transpose(1, 0, 2)
    entries = lax.all_to_all(entries.reshape(peers, owned * slots), "wide", 0, 0, tiled=True)
    entries = entries.reshape(peers * owned, slots)
    column_ids = lax.dynamic_index_in_dim(ids, col, 0, keepdims=False)
    mine = (corner_ids[:, None] == column_ids[None, :]).astype(jnp.float32)
    return jnp.einsum("ps,ks->pk", mine, entries, precision=HIGHEST)


def slots_of_column(ids, amount):
    count = ids.shape[0]
    place = jnp.arange(count, dtype=jnp.int32)
    same = ids[:, None] == ids[None, :]
    first = ~jnp.any(same & (place[None, :] < place[:, None]), axis=1)
    rank_of_first = jnp.sum(first[None, :] & (place[None, :] < place[:, None]), axis=1)
    rank = jnp.sum(jnp.where(same & first[None, :], rank_of_first[None, :], 0), axis=1)
    slots = rank[None, :] == jnp.arange(amount, dtype=jnp.int32)[:, None]
    slot_ids = jnp.max(jnp.where(slots, ids[None, :], 0.0), axis=1)
    return slots.astype(jnp.float32), slot_ids


def body(
    load_table, load_column, face_order, schur, neumann, coarse_basis, corner_map, coarse_inverse
):
    load_table, face_order, schur, neumann, coarse_basis, corner_ids = (
        a[0, 0] for a in (load_table, face_order, schur, neumann, coarse_basis, corner_map)
    )
    patterns = load_table.shape[0]
    prims = corner_ids.shape[0]
    rhs = load_column.shape[0]
    rows_total = lax.axis_size("sub")
    cols_total = lax.axis_size("wide")
    half_slots = rows_total + 1
    selector_full = (face_order[:, None] == jnp.arange(4, dtype=jnp.int32)).astype(jnp.float32)
    selector_half = selector_full.astype(jnp.bfloat16)
    load_select = (load_column[:, None] == jnp.arange(patterns, dtype=jnp.int32)).astype(
        jnp.bfloat16
    )
    load_faces = jnp.einsum(
        "jl,lfn->fjn", load_select, load_table, preferred_element_type=jnp.float32
    )
    row = lax.axis_index("sub")
    col = lax.axis_index("wide")
    inner = jnp.stack([row > 0, row < rows_total - 1, col > 0, col < cols_total - 1])
    weights = jnp.where(inner, jnp.float32(0.5), jnp.float32(1.0))[:, None, None]
    basis = coarse_basis.astype(jnp.float32)
    id_lanes = jnp.broadcast_to(corner_ids.astype(jnp.float32)[:, None], (prims, rhs))
    solution = jnp.zeros(load_faces.shape, jnp.float32)
    for iteration in range(ITERS):
        if iteration == 0:
            residual = assemble(load_faces)
        else:
            residual = assemble(
                load_faces - apply_local(solution, schur, selector_half, selector_full)
            )
        weighted = weights * residual
        restricted = jnp.einsum("pfn,fjn->pj", basis, weighted, precision=HIGHEST)
        in_column = gather(jnp.concatenate([restricted, id_lanes], axis=1), "sub")
        in_column = in_column.reshape(rows_total * prims, 2 * rhs)
        if iteration == 0:
            slots, slot_ids = slots_of_column(in_column[:, rhs], 2 * half_slots)
        summed = jnp.dot(slots, in_column[:, :rhs], precision=HIGHEST)
        summed = jnp.concatenate([summed[:half_slots], summed[half_slots:]], axis=1)
        if iteration == 0:
            id_row = jnp.pad(slot_ids, (0, 2 * rhs - 2 * half_slots))[None, :]
            everyone = gather(jnp.concatenate([summed, id_row]), "wide")
            ids = everyone[:, half_slots, : 2 * half_slots].astype(jnp.int32)
            everyone = everyone[:, :half_slots]
            inverse_rows = own_inverse_rows(corner_ids, ids, coarse_inverse)
            ids = ids.reshape(cols_total, 2, half_slots).transpose(1, 0, 2).reshape(-1)
            rows_at = pick_columns(inverse_rows, ids)
            sent = jnp.concatenate(
                [jnp.broadcast_to(rows_at[None], (4, *rows_at.shape)), basis.transpose(1, 0, 2)], axis=2
            )
            sent = partners(sent)
            partner_basis = sent[:, :, rows_at.shape[1] :]
            rows_at = jnp.concatenate([rows_at[None], sent[:, :, : rows_at.shape[1]]])
            rows_at = rows_at.reshape(5, prims, 2, cols_total * half_slots)
            rows_at = rows_at.transpose(0, 2, 1, 3).reshape(10 * prims, -1)
        else:
            everyone = gather(summed, "wide")
        solved = jnp.dot(
            rows_at, everyone.reshape(cols_total * half_slots, 2 * rhs), precision=HIGHEST
        )
        solved = solved.reshape(5, 2, prims, 2 * rhs)
        picked = solved[:, 0, :, :rhs] + solved[:, 1, :, rhs:]
        neumann_part = apply_local(weighted, neumann, selector_half, selector_full)
        correction = jnp.einsum("pj,pfn->fjn", picked[0], basis, precision=HIGHEST)
        correction += jnp.einsum("fpj,fpn->fjn", picked[1:], partner_basis, precision=HIGHEST)
        update = assemble(weights * neumann_part) + weights * correction
        solution = solution + damping * update
    return solution[None, None]


def solution(mesh):
    in_specs = (
        P("sub", "wide", None, None, None),
        P(),
        P("sub", "wide", None),
        P("sub", "wide", None, None),
        P("sub", "wide", None, None),
        P("sub", "wide", None, None, None),
        P("sub", "wide", None),
        P("wide", None),
    )
    out_specs = P("sub", "wide", None, None, None)
    return jax.shard_map(body, mesh=mesh, in_specs=in_specs, out_specs=out_specs, check_vma=False)
```
